32 devices in a mesh: dp: 4 (over y, z), sp: 8 (over x, core).
Axes of the slice: x: 4, y: 2, z: 2, core: 2. Of those that a mesh axis runs over, the one named last changes fastest.
The devices are a block of a 4x4x8 slice.
Arguments:
- latents: bfloat16 [32, 16, 64, 1280], P('dp', 'sp'), parts along dimension 0
- time_emb: bfloat16 [32, 1280], P('dp'), parts along dimension 0
- context: bfloat16 [32, 77, 768], P('dp'), parts along dimension 0
- res_norm: float32 [2, 2, 2, 1280], replicated
- res_conv_w: bfloat16 [2, 2, 3, 3, 1280, 1280], replicated
- res_conv_b: float32 [2, 2, 1280], replicated
- res_temb_w: bfloat16 [2, 1280, 1280], replicated
- res_temb_b: float32 [2, 1280], replicated
- tr_norm: float32 [2, 1280], replicated
- proj_w: bfloat16 [2, 1280, 1280], replicated
- proj_b: float32 [2, 1280], replicated
- ln_par: float32 [2, 3, 2, 1280], replicated
- self_qkv: bfloat16 [2, 3, 1280, 8, 160], replicated
- cross_q: bfloat16 [2, 1280, 8, 160], replicated
- cross_kv: bfloat16 [2, 2, 768, 8, 160], replicated
- attn_out: bfloat16 [2, 2, 8, 160, 1280], replicated
- attn_b: float32 [2, 2, 1280], replicated
- ff_in_w: bfloat16 [2, 1280, 10240], replicated
- ff_in_b: float32 [2, 10240], replicated
- ff_out_w: bfloat16 [2, 5120, 1280], replicated
- ff_out_b: float32 [2, 1280], replicated
Outputs:
- output: bfloat16 [32, 16, 64, 1280], P('dp', 'sp'), parts along dimension 0
There are 4 independent parts. The reference program is written for one: setup_inputs(seed, part) draws one part's arguments, and reference() takes and returns one part's arrays. A program takes and returns all parts, laid end to end along the dimension named above; an argument that names none is the same for every part.
All inputs are finite; a program needn't handle non-finite values.
Results may differ from the reference program's by a relative error of at most 0.0196095.
Values are sent between devices in bfloat16 or wider.
A program may use at most 768 MiB of HBM per device.

```python
import math
import jax
import jax.numpy as jnp
from jax import lax

IMG_BATCH = 8
IMG_ROWS = 16
IMG_WIDTH = 64
CHANNELS = 1280
NUM_HEADS = 8
TIME_DIM = 1280
CTX_DIM = 768
CTX_LEN = 77
NUM_GROUPS = 32
FF_DIM = 5120

NUM_TOKENS = IMG_ROWS * IMG_WIDTH
HEAD_DIM = CHANNELS // NUM_HEADS
ATTN_SCALE = 1.0 / math.sqrt(HEAD_DIM)


def scaled_normal(rng_key, arr_shape, fan_in):
    return jax.random.normal(rng_key, arr_shape, jnp.float32) / math.sqrt(fan_in)


def setup_inputs(seed: int = 0, part: int = 0) -> dict:
    part_keys = jax.random.split(jax.random.fold_in(jax.random.key(seed + 1), part), 6)
    wt_keys = jax.random.split(jax.random.key(seed), 18)
    row_pos = jnp.arange(IMG_ROWS, dtype=jnp.float32)[None, :, None, None] * (math.pi / IMG_ROWS)
    mean_phase = jnp.repeat(jax.random.uniform(part_keys[0], (IMG_BATCH, 1, 1, NUM_GROUPS), jnp.float32, 0.0, 2.0 * math.pi), CHANNELS // NUM_GROUPS, axis=-1)
    scale_phase = jax.random.uniform(part_keys[1], (IMG_BATCH, 1, 1, CHANNELS), jnp.float32, 0.0, 2.0 * math.pi)
    chan_shift = 0.3 * jax.random.normal(part_keys[2], (IMG_BATCH, 1, 1, CHANNELS), jnp.float32)
    noise_val = jax.random.normal(part_keys[3], (IMG_BATCH, IMG_ROWS, IMG_WIDTH, CHANNELS), jnp.float32)
    latents = noise_val * (1.0 + 0.5 * jnp.cos(row_pos + scale_phase)) + 0.8 * jnp.sin(row_pos + mean_phase) + chan_shift
    time_emb = jax.random.normal(part_keys[4], (IMG_BATCH, TIME_DIM), jnp.float32)
    context = jax.random.normal(part_keys[5], (IMG_BATCH, CTX_LEN, CTX_DIM), jnp.float32)
    sharp_self = 0.8 * math.sqrt(math.log(NUM_TOKENS))
    sharp_cross = 0.8 * math.sqrt(math.log(CTX_LEN))
    affine_base = jnp.array([1.0, 0.0], jnp.float32)[:, None]
    qkv_gain = jnp.array([sharp_self, 1.0, 2.0], jnp.float32)[:, None, None, None]
    kv_gain = jnp.array([1.0, 2.0], jnp.float32)[:, None, None, None]
    return {
        'latents': latents.astype(jnp.bfloat16),
        'time_emb': time_emb.astype(jnp.bfloat16),
        'context': context.astype(jnp.bfloat16),
        'res_norm': affine_base + 0.25 * jax.random.normal(wt_keys[0], (2, 2, 2, CHANNELS), jnp.float32),
        'res_conv_w': scaled_normal(wt_keys[1], (2, 2, 3, 3, CHANNELS, CHANNELS), 9 * CHANNELS).astype(jnp.bfloat16),
        'res_conv_b': 0.3 * jax.random.normal(wt_keys[2], (2, 2, CHANNELS), jnp.float32),
        'res_temb_w': scaled_normal(wt_keys[3], (2, TIME_DIM, CHANNELS), TIME_DIM).astype(jnp.bfloat16),
        'res_temb_b': 0.3 * jax.random.normal(wt_keys[4], (2, CHANNELS), jnp.float32),
        'tr_norm': affine_base + 0.25 * jax.random.normal(wt_keys[5], (2, CHANNELS), jnp.float32),
        'proj_w': scaled_normal(wt_keys[6], (2, CHANNELS, CHANNELS), CHANNELS).astype(jnp.bfloat16),
        'proj_b': 0.3 * jax.random.normal(wt_keys[7], (2, CHANNELS), jnp.float32),
        'ln_par': affine_base + 0.25 * jax.random.normal(wt_keys[8], (2, 3, 2, CHANNELS), jnp.float32),
        'self_qkv': (scaled_normal(wt_keys[9], (2, 3, CHANNELS, NUM_HEADS, HEAD_DIM), CHANNELS) * qkv_gain).astype(jnp.bfloat16),
        'cross_q': (scaled_normal(wt_keys[10], (2, CHANNELS, NUM_HEADS, HEAD_DIM), CHANNELS) * sharp_cross).astype(jnp.bfloat16),
        'cross_kv': (scaled_normal(wt_keys[11], (2, 2, CTX_DIM, NUM_HEADS, HEAD_DIM), CTX_DIM) * kv_gain).astype(jnp.bfloat16),
        'attn_out': scaled_normal(wt_keys[12], (2, 2, NUM_HEADS, HEAD_DIM, CHANNELS), CHANNELS).astype(jnp.bfloat16),
        'attn_b': 0.3 * jax.random.normal(wt_keys[13], (2, 2, CHANNELS), jnp.float32),
        'ff_in_w': scaled_normal(wt_keys[14], (2, CHANNELS, 2 * FF_DIM), CHANNELS).astype(jnp.bfloat16),
        'ff_in_b': 0.3 * jax.random.normal(wt_keys[15], (2, 2 * FF_DIM), jnp.float32),
        'ff_out_w': scaled_normal(wt_keys[16], (2, FF_DIM, CHANNELS), FF_DIM).astype(jnp.bfloat16),
        'ff_out_b': 0.3 * jax.random.normal(wt_keys[17], (2, CHANNELS), jnp.float32),
    }


def matmul_f32(form, left, right):
    return jnp.einsum(form, left.astype(jnp.float32), right.astype(jnp.float32))


def group_norm(values, norm_gain, norm_bias, eps_val):
    grouped = values.astype(jnp.float32).reshape(IMG_BATCH, IMG_ROWS, IMG_WIDTH, NUM_GROUPS, CHANNELS // NUM_GROUPS)
    grp_mean = grouped.mean(axis=(1, 2, 4), keepdims=True)
    grp_sq = (grouped * grouped).mean(axis=(1, 2, 4), keepdims=True)
    normed = (grouped - grp_mean) * lax.rsqrt(grp_sq - grp_mean * grp_mean + eps_val)
    return normed.reshape(IMG_BATCH, IMG_ROWS, IMG_WIDTH, CHANNELS) * norm_gain + norm_bias


def conv_same(act_in, kernel):
    return lax.conv_general_dilated(act_in.astype(jnp.float32), kernel.astype(jnp.float32), (1, 1), 'SAME', dimension_numbers=('NHWC', 'HWIO', 'NHWC'))


def resnet(latents, time_emb, res_index, res_norm, res_conv_w, res_conv_b, res_temb_w, res_temb_b):
    first_act = jax.nn.silu(group_norm(latents, res_norm[res_index, 0, 0], res_norm[res_index, 0, 1], 1e-5)).astype(jnp.bfloat16)
    time_proj = jnp.dot(jax.nn.silu(time_emb.astype(jnp.float32)).astype(jnp.bfloat16), res_temb_w[res_index], preferred_element_type=jnp.float32) + res_temb_b[res_index]
    hidden = (conv_same(first_act, res_conv_w[res_index, 0]) + res_conv_b[res_index, 0] + time_proj[:, None, None, :]).astype(jnp.bfloat16)
    second_act = jax.nn.silu(group_norm(hidden, res_norm[res_index, 1, 0], res_norm[res_index, 1, 1], 1e-5)).astype(jnp.bfloat16)
    update = conv_same(second_act, res_conv_w[res_index, 1]) + res_conv_b[res_index, 1]
    return (latents.astype(jnp.float32) + update).astype(jnp.bfloat16)


def layer_norm(values, norm_gain, norm_bias):
    centered = values.astype(jnp.float32)
    centered = centered - centered.mean(axis=-1, keepdims=True)
    variance = (centered * centered).mean(axis=-1, keepdims=True)
    return (centered * lax.rsqrt(variance + 1e-5) * norm_gain + norm_bias).astype(jnp.bfloat16)


def attend_block(q_blk, k_all, v_all):
    scores = matmul_f32('bqhd,bkhd->bhqk', q_blk, k_all) * ATTN_SCALE
    row_exp = jnp.exp(scores - scores.max(axis=-1, keepdims=True))
    row_sum = row_exp.sum(axis=-1)
    row_out = matmul_f32('bhqk,bkhd->bqhd', row_exp.astype(jnp.bfloat16), v_all)
    return (row_out / jnp.swapaxes(row_sum, 1, 2)[..., None]).astype(jnp.bfloat16)


def transformer(hidden, context, tr_norm, proj_w, proj_b, ln_par, self_qkv, cross_q, cross_kv, attn_out, attn_b, ff_in_w, ff_in_b, ff_out_w, ff_out_b):
    normed = group_norm(hidden, tr_norm[0], tr_norm[1], 1e-6).astype(jnp.bfloat16).reshape(IMG_BATCH, NUM_TOKENS, CHANNELS)
    hidden_tok = (matmul_f32('bnc,cd->bnd', normed, proj_w[0]) + proj_b[0]).astype(jnp.bfloat16)

    def block_fn(carried, layer_w):
        ln_w, qkv_w, cq_w, ckv_w, out_w, out_b, ffi_w, ffi_b, ffo_w, ffo_b = layer_w
        normed_one = layer_norm(carried, ln_w[0, 0], ln_w[0, 1])
        q_all = matmul_f32('bnc,chd->bnhd', normed_one, qkv_w[0]).astype(jnp.bfloat16)
        k_all = matmul_f32('bnc,chd->bnhd', normed_one, qkv_w[1]).astype(jnp.bfloat16)
        v_all = matmul_f32('bnc,chd->bnhd', normed_one, qkv_w[2]).astype(jnp.bfloat16)
        q_rows = jnp.swapaxes(q_all.reshape(IMG_BATCH, IMG_ROWS, IMG_WIDTH, NUM_HEADS, HEAD_DIM), 0, 1)
        attended = lax.map(lambda q_row: attend_block(q_row, k_all, v_all), q_rows)
        attended = jnp.swapaxes(attended, 0, 1).reshape(IMG_BATCH, NUM_TOKENS, NUM_HEADS, HEAD_DIM)
        carried = (carried.astype(jnp.float32) + matmul_f32('bnhd,hdc->bnc', attended, out_w[0]) + out_b[0]).astype(jnp.bfloat16)
        normed_two = layer_norm(carried, ln_w[1, 0], ln_w[1, 1])
        q_cross = matmul_f32('bnc,chd->bnhd', normed_two, cq_w).astype(jnp.bfloat16)
        k_cross = matmul_f32('btc,chd->bthd', context, ckv_w[0]).astype(jnp.bfloat16)
        v_cross = matmul_f32('btc,chd->bthd', context, ckv_w[1]).astype(jnp.bfloat16)
        crossed = attend_block(q_cross, k_cross, v_cross)
        carried = (carried.astype(jnp.float32) + matmul_f32('bnhd,hdc->bnc', crossed, out_w[1]) + out_b[1]).astype(jnp.bfloat16)
        normed_three = layer_norm(carried, ln_w[2, 0], ln_w[2, 1])
        ff_proj = matmul_f32('bnc,cf->bnf', normed_three, ffi_w) + ffi_b
        gated_act = (ff_proj[..., :FF_DIM] * jax.nn.gelu(ff_proj[..., FF_DIM:], approximate=False)).astype(jnp.bfloat16)
        carried = (carried.astype(jnp.float32) + matmul_f32('bnf,fc->bnc', gated_act, ffo_w) + ffo_b).astype(jnp.bfloat16)
        return carried, None

    hidden_tok, _unused = lax.scan(block_fn, hidden_tok, (ln_par, self_qkv, cross_q, cross_kv, attn_out, attn_b, ff_in_w, ff_in_b, ff_out_w, ff_out_b))
    out_tok = matmul_f32('bnc,cd->bnd', hidden_tok, proj_w[1]) + proj_b[1] + hidden.reshape(IMG_BATCH, NUM_TOKENS, CHANNELS).astype(jnp.float32)
    return out_tok.astype(jnp.bfloat16).reshape(IMG_BATCH, IMG_ROWS, IMG_WIDTH, CHANNELS)


def reference(latents, time_emb, context, res_norm, res_conv_w, res_conv_b, res_temb_w, res_temb_b, tr_norm, proj_w, proj_b, ln_par, self_qkv, cross_q, cross_kv, attn_out, attn_b, ff_in_w, ff_in_b, ff_out_w, ff_out_b):
    first_out = resnet(latents, time_emb, 0, res_norm, res_conv_w, res_conv_b, res_temb_w, res_temb_b)
    middle = transformer(first_out, context, tr_norm, proj_w, proj_b, ln_par, self_qkv, cross_q, cross_kv, attn_out, attn_b, ff_in_w, ff_in_b, ff_out_w, ff_out_b)
    return resnet(middle, time_emb, 1, res_norm, res_conv_w, res_conv_b, res_temb_w, res_temb_b)
```

```python
import functools
import math
import jax
import jax.numpy as jnp
from jax import lax
from jax.experimental import pallas as pl
from jax.experimental.pallas import tpu as pltpu
from jax.sharding import PartitionSpec as P

NUM_GROUPS = 32
LANES = 128
VMEM_LIMIT = 60 * 1024 * 1024
LOG2_E = 1.4426950408889634
MESH_ID = pl.DeviceIdType.MESH


def swap_kernel(x_ref, o_ref, *rest, sp_size, with_stats):
    if with_stats:
        stat_ref, send_sems, recv_sems = rest
    else:
        send_sems, recv_sems = rest
    me = lax.axis_index('sp')
    barrier = pltpu.get_barrier_semaphore()
    for step in range(1, sp_size):
        pl.semaphore_signal(barrier, inc=1, device_id={'sp': lax.rem(me + step, sp_size)}, device_id_type=MESH_ID)
    pl.semaphore_wait(barrier, sp_size - 1)
    copies = []
    for step in range(1, sp_size):
        peer = lax.rem(me + step, sp_size)
        copy = pltpu.make_async_remote_copy(
            src_ref=x_ref.at[peer], dst_ref=o_ref.at[me], send_sem=send_sems.at[step], recv_sem=recv_sems.at[step],
            device_id={'sp': peer}, device_id_type=MESH_ID)
        copy.start()
        copies.append(copy)
    own = x_ref[me]
    o_ref[me] = own
    if with_stats:
        vals = own.astype(jnp.float32)
        sums, squares = vals.sum(axis=0, keepdims=True), (vals * vals).sum(axis=0, keepdims=True)
    for step in range(1, sp_size):
        copies[step - 1].wait_recv()
        if with_stats:
            vals = o_ref[lax.rem(me + sp_size - step, sp_size)].astype(jnp.float32)
            sums = sums + vals.sum(axis=0, keepdims=True)
            squares = squares + (vals * vals).sum(axis=0, keepdims=True)
    if with_stats:
        stat_ref[0:1] = sums
        stat_ref[1:2] = squares
    for copy in copies:
        copy.wait_send()


def swap(bands, sp_size, with_stats, collective_id):
    _, tok_n, chan_n = bands.shape
    out_shape = [jax.ShapeDtypeStruct(bands.shape, bands.dtype)]
    if with_stats:
        out_shape.append(jax.ShapeDtypeStruct((2, chan_n), jnp.float32))
    vmem = pl.BlockSpec(memory_space=pltpu.VMEM)
    return pl.pallas_call(
        functools.partial(swap_kernel, sp_size=sp_size, with_stats=with_stats),
        out_shape=out_shape,
        in_specs=[vmem],
        out_specs=[vmem] * len(out_shape),
        scratch_shapes=[pltpu.SemaphoreType.DMA((sp_size,)), pltpu.SemaphoreType.DMA((sp_size,))],
        compiler_params=pltpu.CompilerParams(collective_id=collective_id, has_side_effects=True),
        name='swap',
    )(bands)


def group_affine(sums, squares, count_n, gain, bias, eps_val):
    chan_n = sums.shape[0]
    width = chan_n // NUM_GROUPS
    mean = sums.reshape(NUM_GROUPS, width).sum(axis=1) / count_n
    var = squares.reshape(NUM_GROUPS, width).sum(axis=1) / count_n - mean * mean
    inv_std = lax.rsqrt(var + eps_val)
    return jnp.repeat(mean, width), jnp.repeat(inv_std, width) * gain, bias


def chan_stats(values):
    vals = values.astype(jnp.float32)
    axes = tuple(range(vals.ndim - 1))
    return vals.sum(axis=axes), (vals * vals).sum(axis=axes)


def group_norm(values, stats, gain, bias, eps_val):
    count_n = values.size // NUM_GROUPS
    mean, scale, shift = group_affine(stats[0], stats[1], count_n, gain, bias, eps_val)
    return (values.astype(jnp.float32) - mean) * scale + shift


def conv_bands(act, kernel):
    edge = jnp.zeros_like(act[:1, :1])
    from_above = jnp.concatenate([edge, act[:-1, -1:]], axis=0)
    from_below = jnp.concatenate([act[1:, :1], edge], axis=0)
    padded = jnp.concatenate([from_above, act, from_below], axis=1)
    return lax.conv_general_dilated(padded, kernel, (1, 1), ((0, 0), (1, 1)), dimension_numbers=('NHWC', 'HWIO', 'NHWC'), preferred_element_type=jnp.float32)


def resnet(values, stats, time_row, r, res_norm, res_conv_w, res_conv_b, res_temb_w, res_temb_b):
    first_act = jax.nn.silu(group_norm(values, stats, res_norm[r, 0, 0], res_norm[r, 0, 1], 1e-5)).astype(jnp.bfloat16)
    time_act = jax.nn.silu(time_row.astype(jnp.float32)).astype(jnp.bfloat16)
    time_proj = jnp.dot(time_act, res_temb_w[r], preferred_element_type=jnp.float32)[0] + res_temb_b[r]
    hidden = (conv_bands(first_act, res_conv_w[r, 0]) + res_conv_b[r, 0] + time_proj).astype(jnp.bfloat16)
    second_act = jax.nn.silu(group_norm(hidden, chan_stats(hidden), res_norm[r, 1, 0], res_norm[r, 1, 1], 1e-5)).astype(jnp.bfloat16)
    update = conv_bands(second_act, res_conv_w[r, 1]) + res_conv_b[r, 1]
    return (values.astype(jnp.float32) + update).astype(jnp.bfloat16)


def dot_t(left, right):
    return lax.dot_general(left, right, (((1,), (1,)), ((), ())), preferred_element_type=jnp.float32)


def dot_n(left, right):
    return jnp.dot(left, right, preferred_element_type=jnp.float32)


def layer_norm_rows(values, gain, bias):
    vals = values.astype(jnp.float32)
    vals = vals - vals.mean(axis=-1, keepdims=True)
    var = (vals * vals).mean(axis=-1, keepdims=True)
    return (vals * lax.rsqrt(var + 1e-5) * gain + bias).astype(jnp.bfloat16)


def each_block(tok_n, block, body):
    def step(index, carry):
        body(pl.ds(pl.multiple_of(index * block, block), block))
        return carry
    lax.fori_loop(0, tok_n // block, step, 0)


def head_window(head, dim_n):
    start = head * dim_n
    low = start // LANES * LANES
    high = -(-(start + dim_n) // LANES) * LANES
    return low, high, start - low


def lane_mask(rows_n, width, offset, dim_n):
    lane = lax.broadcasted_iota(jnp.int32, (rows_n, width), 1)
    return (lane >= offset) & (lane < offset + dim_n)


def put_head(o_ref, rows, low, high, offset, dim_n, value):
    if offset:
        lane = lax.broadcasted_iota(jnp.int32, (value.shape[0], LANES), 1)
        o_ref[rows, low:low + LANES] = jnp.where(lane >= offset, value[:, :LANES].astype(jnp.float32), o_ref[rows, low:low + LANES].astype(jnp.float32)).astype(o_ref.dtype)
        o_ref[rows, low + LANES:high] = value[:, LANES:].astype(o_ref.dtype)
    else:
        o_ref[rows, low:high] = value.astype(o_ref.dtype)


def qkv_kernel(u_ref, ln_ref, w_ref, o_ref, n_ref):
    @pl.when(pl.program_id(0) == 0)
    def _():
        def norm(rows):
            n_ref[rows] = layer_norm_rows(u_ref[rows], ln_ref[0, 0:1], ln_ref[0, 1:2])
        each_block(u_ref.shape[0], 64, norm)
    o_ref[...] = dot_t(n_ref[...], w_ref[...]).astype(o_ref.dtype)


def qkv_call(u, ln_par, w, layer, chunk=768):
    tok_n, chan_n = u.shape
    wide = w.shape[1]
    return pl.pallas_call(
        qkv_kernel,
        grid=(wide // chunk,),
        out_shape=jax.ShapeDtypeStruct((tok_n, wide), jnp.bfloat16),
        in_specs=[
            pl.BlockSpec((tok_n, chan_n), lambda j: (0, 0)),
            pl.BlockSpec((None, 3, 2, chan_n), lambda j: (layer, 0, 0, 0)),
            pl.BlockSpec((None, chunk, chan_n), lambda j: (layer, j, 0)),
        ],
        out_specs=pl.BlockSpec((tok_n, chunk), lambda j: (0, j)),
        scratch_shapes=[pltpu.VMEM((tok_n, chan_n), jnp.bfloat16)],
        compiler_params=pltpu.CompilerParams(vmem_limit_bytes=VMEM_LIMIT),
        cost_estimate=pl.CostEstimate(flops=2 * tok_n * chan_n * wide, bytes_accessed=2 * (wide * chan_n + tok_n * chan_n + tok_n * wide), transcendentals=0),
        name='qkv',
    )(u, ln_par, w)


def attend_kernel(q_ref, k_ref, v_ref, o_ref, *, heads, dim_n, block):
    tok_n = q_ref.shape[0]
    scale = LOG2_E / math.sqrt(dim_n)

    def rows_step(rows):
        for head in range(heads):
            low, high, offset = head_window(head, dim_n)
            queries = jnp.where(lane_mask(block, high - low, offset, dim_n), q_ref[rows, low:high], jnp.zeros((), q_ref.dtype))
            scores = dot_t(queries, k_ref[:, low:high])
            top = scores.max(axis=-1, keepdims=True)
            expo = jnp.exp2((scores - top) * scale)
            total = expo.sum(axis=-1, keepdims=True)
            out = dot_n(expo.astype(jnp.bfloat16), v_ref[:, low:high]) * (1.0 / total)
            put_head(o_ref, rows, low, high, offset, dim_n, out)

    each_block(tok_n, block, rows_step)


def attend_call(qkv, head_n, dim_n, block=256):
    tok_n = qkv.shape[0]
    heads = LANES // math.gcd(LANES, dim_n)
    width = heads * dim_n
    groups = head_n // heads
    return pl.pallas_call(
        functools.partial(attend_kernel, heads=heads, dim_n=dim_n, block=block),
        grid=(groups,),
        out_shape=jax.ShapeDtypeStruct((tok_n, head_n * dim_n), jnp.bfloat16),
        in_specs=[
            pl.BlockSpec((tok_n, width), lambda g: (0, g)),
            pl.BlockSpec((tok_n, width), lambda g: (0, groups + g)),
            pl.BlockSpec((tok_n, width), lambda g: (0, 2 * groups + g)),
        ],
        out_specs=pl.BlockSpec((tok_n, width), lambda g: (0, g)),
        compiler_params=pltpu.CompilerParams(vmem_limit_bytes=VMEM_LIMIT),
        cost_estimate=pl.CostEstimate(flops=4 * tok_n * tok_n * head_n * dim_n, bytes_accessed=8 * tok_n * head_n * dim_n, transcendentals=head_n * tok_n * tok_n),
        name='attend',
    )(qkv, qkv, qkv)


def cross_kernel(u_ref, a_ref, ln_ref, wo_ref, bo_ref, wq_ref, k_ref, v_ref, out_ref, q_ref, c_ref, *, head_n, dim_n, key_n):
    carried = (u_ref[...].astype(jnp.float32) + dot_n(a_ref[...], wo_ref[0]) + bo_ref[0:1]).astype(jnp.bfloat16)
    q_ref[...] = dot_t(layer_norm_rows(carried, ln_ref[1, 0:1], ln_ref[1, 1:2]), wq_ref[...]).astype(jnp.bfloat16)
    rows_n = carried.shape[0]
    pad_n = k_ref.shape[0]
    scale = LOG2_E / math.sqrt(dim_n)
    live = lax.broadcasted_iota(jnp.int32, (rows_n, pad_n), 1) < key_n
    for head in range(head_n):
        low, high, offset = head_window(head, dim_n)
        keys = jnp.where(lane_mask(pad_n, high - low, offset, dim_n), k_ref[:, low:high], jnp.zeros((), k_ref.dtype))
        scores = jnp.where(live, dot_t(q_ref[:, low:high], keys), -jnp.inf)
        top = scores.max(axis=-1, keepdims=True)
        expo = jnp.exp2((scores - top) * scale)
        total = expo.sum(axis=-1, keepdims=True)
        out = dot_n(expo.astype(jnp.bfloat16), v_ref[:, low:high]) * (1.0 / total)
        put_head(c_ref, slice(None), low, high, offset, dim_n, out)
    out_ref[...] = (carried.astype(jnp.float32) + dot_n(c_ref[...], wo_ref[1]) + bo_ref[1:2]).astype(jnp.bfloat16)


def cross_call(u, attended, ln_par, attn_out, attn_b, cross_q, kv, layer, head_n, dim_n, key_n, block=256):
    tok_n, chan_n = u.shape
    wide = head_n * dim_n
    pad_n = kv.shape[0]
    return pl.pallas_call(
        functools.partial(cross_kernel, head_n=head_n, dim_n=dim_n, key_n=key_n),
        grid=(tok_n // block,),
        out_shape=jax.ShapeDtypeStruct((tok_n, chan_n), jnp.bfloat16),
        in_specs=[
            pl.BlockSpec((block, chan_n), lambda i: (i, 0)),
            pl.BlockSpec((block, wide), lambda i: (i, 0)),
            pl.BlockSpec((None, 3, 2, chan_n), lambda i: (layer, 0, 0, 0)),
            pl.BlockSpec((None, 2, wide, chan_n), lambda i: (layer, 0, 0, 0)),
            pl.BlockSpec((None, 2, chan_n), lambda i: (layer, 0, 0)),
            pl.BlockSpec((None, wide, chan_n), lambda i: (layer, 0, 0)),
            pl.BlockSpec((pad_n, wide), lambda i: (0, 2 * layer)),
            pl.BlockSpec((pad_n, wide), lambda i: (0, 2 * layer + 1)),
        ],
        out_specs=pl.BlockSpec((block, chan_n), lambda i: (i, 0)),
        scratch_shapes=[pltpu.VMEM((block, wide), jnp.bfloat16), pltpu.VMEM((block, wide), jnp.bfloat16)],
        compiler_params=pltpu.CompilerParams(vmem_limit_bytes=VMEM_LIMIT),
        cost_estimate=pl.CostEstimate(flops=6 * tok_n * chan_n * wide + 4 * tok_n * pad_n * wide, bytes_accessed=6 * wide * chan_n + 6 * tok_n * chan_n, transcendentals=head_n * tok_n * pad_n),
        name='cross',
    )(u, attended, ln_par, attn_out, attn_b, cross_q, kv, kv)


def ff_kernel(u_ref, ln_ref, wa_ref, wb_ref, ba_ref, bb_ref, w2_ref, b2_ref, o_ref, n_ref, acc_ref, *, layer, block):
    step = pl.program_id(0)
    tok_n = u_ref.shape[0]

    @pl.when(step == 0)
    def _():
        def norm(rows):
            n_ref[rows] = layer_norm_rows(u_ref[rows], ln_ref[2, 0:1], ln_ref[2, 1:2])
            acc_ref[rows] = u_ref[rows].astype(jnp.float32) + b2_ref[layer:layer + 1]
        each_block(tok_n, 64, norm)

    def gate(start):
        rows = pl.ds(start, block)
        first = dot_n(n_ref[rows], wa_ref[...]) + ba_ref[layer:layer + 1]
        second = dot_n(n_ref[rows], wb_ref[...]) + bb_ref[layer:layer + 1]
        return (first * (0.5 * second * (1.0 + lax.erf(second * math.sqrt(0.5))))).astype(jnp.bfloat16)

    def add(start, gated):
        rows = pl.ds(start, block)
        acc_ref[rows] += dot_n(gated, w2_ref[...])

    starts = list(range(0, tok_n, block))
    held = gate(starts[0])
    for index, start in enumerate(starts):
        following = gate(starts[index + 1]) if index + 1 < len(starts) else None
        add(start, held)
        held = following

    @pl.when(step == pl.num_programs(0) - 1)
    def _():
        def done(rows):
            o_ref[rows] = acc_ref[rows].astype(o_ref.dtype)
        each_block(tok_n, 64, done)


def ff_call(u, ln_par, ff_in_w, ff_in_b, ff_out_w, ff_out_b, layer, chunk=512, block=256):
    tok_n, chan_n = u.shape
    width = ff_out_w.shape[1]
    steps = width // chunk
    layers = ff_in_b.shape[0]
    return pl.pallas_call(
        functools.partial(ff_kernel, layer=layer, block=block),
        grid=(steps,),
        out_shape=jax.ShapeDtypeStruct((tok_n, chan_n), jnp.bfloat16),
        in_specs=[
            pl.BlockSpec((tok_n, chan_n), lambda j: (0, 0)),
            pl.BlockSpec((None, 3, 2, chan_n), lambda j: (layer, 0, 0, 0)),
            pl.BlockSpec((None, chan_n, chunk), lambda j: (layer, 0, j)),
            pl.BlockSpec((None, chan_n, chunk), lambda j: (layer, 0, steps + j)),
            pl.BlockSpec((layers, chunk), lambda j: (0, j)),
            pl.BlockSpec((layers, chunk), lambda j: (0, steps + j)),
            pl.BlockSpec((None, chunk, chan_n), lambda j: (layer, j, 0)),
            pl.BlockSpec((layers, chan_n), lambda j: (0, 0)),
        ],
        out_specs=pl.BlockSpec((tok_n, chan_n), lambda j: (0, 0)),
        scratch_shapes=[pltpu.VMEM((tok_n, chan_n), jnp.bfloat16), pltpu.VMEM((tok_n, chan_n), jnp.float32)],
        compiler_params=pltpu.CompilerParams(vmem_limit_bytes=VMEM_LIMIT),
        cost_estimate=pl.CostEstimate(flops=6 * tok_n * chan_n * width, bytes_accessed=6 * chan_n * width + 4 * tok_n * chan_n, transcendentals=tok_n * width),
        name='ff',
    )(u, ln_par, ff_in_w, ff_in_w, ff_in_b, ff_in_b, ff_out_w, ff_out_b)


def transformer(hidden, context_row, tr_norm, proj_w, proj_b, ln_par, self_qkv, cross_q, cross_kv, attn_out, attn_b, ff_in_w, ff_in_b, ff_out_w, ff_out_b):
    layers, _, chan_n, head_n, dim_n = self_qkv.shape
    wide = head_n * dim_n
    key_n = context_row.shape[0]
    qkv_w = jnp.transpose(self_qkv, (0, 1, 3, 4, 2)).reshape(layers, 3 * wide, chan_n)
    crq_w = jnp.transpose(cross_q, (0, 2, 3, 1)).reshape(layers, wide, chan_n)
    ckv_w = jnp.transpose(cross_kv, (0, 1, 3, 4, 2)).reshape(layers * 2 * wide, cross_kv.shape[2])
    out_w = attn_out.reshape(layers, 2, wide, chan_n)
    pad_n = -(-key_n // LANES) * LANES
    padded = jnp.pad(context_row, ((0, pad_n - key_n), (0, 0)))
    kv = dot_t(padded, ckv_w).astype(jnp.bfloat16)
    normed = group_norm(hidden, chan_stats(hidden), tr_norm[0], tr_norm[1], 1e-6).astype(jnp.bfloat16)
    u = (dot_n(normed, proj_w[0]) + proj_b[0]).astype(jnp.bfloat16)
    for layer in range(layers):
        qkv = qkv_call(u, ln_par, qkv_w, layer)
        attended = attend_call(qkv, head_n, dim_n)
        u = cross_call(u, attended, ln_par, out_w, attn_b, crq_w, kv, layer, head_n, dim_n, key_n)
        u = ff_call(u, ln_par, ff_in_w, ff_in_b, ff_out_w, ff_out_b, layer)
    return (dot_n(u, proj_w[1]) + proj_b[1] + hidden.astype(jnp.float32)).astype(jnp.bfloat16)


def device_block(latents, time_emb, context, res_norm, res_conv_w, res_conv_b, res_temb_w, res_temb_b, tr_norm, proj_w, proj_b, ln_par, self_qkv, cross_q, cross_kv, attn_out, attn_b, ff_in_w, ff_in_b, ff_out_w, ff_out_b, sp_size):
    batch_n, band_n, cols_n, chan_n = latents.shape
    rows_n = band_n * sp_size
    me = lax.axis_index('sp')
    time_row = lax.dynamic_slice_in_dim(time_emb, me, 1, axis=0)
    context_row = lax.dynamic_index_in_dim(context, me, axis=0, keepdims=False)
    whole, stats = swap(latents.reshape(batch_n, band_n * cols_n, chan_n), sp_size, True, 0)
    values = whole.reshape(sp_size, band_n, cols_n, chan_n)
    first = resnet(values, stats, time_row, 0, res_norm, res_conv_w, res_conv_b, res_temb_w, res_temb_b)
    middle = transformer(first.reshape(rows_n * cols_n, chan_n), context_row, tr_norm, proj_w, proj_b, ln_par, self_qkv, cross_q, cross_kv, attn_out, attn_b, ff_in_w, ff_in_b, ff_out_w, ff_out_b).reshape(values.shape)
    last = resnet(middle, chan_stats(middle), time_row, 1, res_norm, res_conv_w, res_conv_b, res_temb_w, res_temb_b)
    bands = swap(last.reshape(sp_size, band_n * cols_n, chan_n), sp_size, False, 1)[0]
    return bands.reshape(batch_n, band_n, cols_n, chan_n)


def solution(mesh):
    sp_size = mesh.shape['sp']
    row_spec = P('dp', 'sp')
    part_spec = P('dp')
    in_specs = (row_spec, part_spec, part_spec) + (P(),) * 18
    body_fn = functools.partial(device_block, sp_size=sp_size)
    return jax.shard_map(body_fn, mesh=mesh, in_specs=in_specs, out_specs=row_spec, check_vma=False)
```
